16 devices in a mesh: rep: 1, dp: 16 (over x, y, z, core).
Axes of the slice: x: 2, y: 2, z: 2, core: 2. Of those that a mesh axis runs over, the one named last changes fastest.
Arguments:
- x: bfloat16 [16, 2048, 1280], P(('rep', 'dp'))
- dy: bfloat16 [16, 2048, 1280], P(('rep', 'dp'))
- w_gate: bfloat16 [2, 1280, 4096], replicated
- w_up: bfloat16 [2, 1280, 4096], replicated
- w_down: bfloat16 [2, 4096, 1280], replicated
- m_w_gate: float32 [2, 1280, 4096], P(None, 'dp')
- m_w_up: float32 [2, 1280, 4096], P(None, 'dp')
- m_w_down: float32 [2, 4096, 1280], P(None, 'dp')
- v_w_gate: float32 [2, 1280, 4096], P(None, 'dp')
- v_w_up: float32 [2, 1280, 4096], P(None, 'dp')
- v_w_down: float32 [2, 4096, 1280], P(None, 'dp')
Outputs:
- output 1: bfloat16 [2, 1280, 4096], P('rep')
- output 2: bfloat16 [2, 1280, 4096], P('rep')
- output 3: bfloat16 [2, 4096, 1280], P('rep')
- output 4: float32 [2, 1280, 4096], P('rep', 'dp')
- output 5: float32 [2, 1280, 4096], P('rep', 'dp')
- output 6: float32 [2, 4096, 1280], P('rep', 'dp')
- output 7: float32 [2, 1280, 4096], P('rep', 'dp')
- output 8: float32 [2, 1280, 4096], P('rep', 'dp')
- output 9: float32 [2, 4096, 1280], P('rep', 'dp')
All inputs are finite; a program needn't handle non-finite values.
Results may differ from the reference program's by a relative error of at most 0.022.
Values are sent between devices in bfloat16 or wider.
A program may use at most 2 GiB of HBM per device.

```python
import jax
import jax.numpy as jnp
from jax import lax

SEQUENCES = 16
TOKENS = 2048
D = 1280
FF = 4096
LAYERS = 2
NAMES = ("w_gate", "w_up", "w_down")
SHAPES = {"w_gate": (LAYERS, D, FF), "w_up": (LAYERS, D, FF), "w_down": (LAYERS, FF, D)}


def bump(key, n, height):
    away = (jnp.arange(n, dtype=jnp.int32) - jax.random.randint(key, (), 0, n, jnp.int32)) % n
    return jnp.where(away < n // 8, height, 1.0)


def together(key, own, strength):
    shared = jax.random.normal(key, own.shape[1:], jnp.float32)
    return (own + strength * shared) * lax.rsqrt(1 + strength * strength)


def setup_inputs(seed: int = 0, part: int = 0) -> dict:
    kx, kdy, ka, kb, kz, kf, kh, kl, *keys = jax.random.split(jax.random.key(seed), 8 + 3 * len(NAMES))
    kx, kdy, ka, kb = (jax.random.fold_in(k, part) for k in (kx, kdy, ka, kb))
    kw, km, kv = (keys[i::3] for i in range(3))
    shape = (SEQUENCES, TOKENS, D)
    much_x, much_dy = jax.random.uniform(kz, (2,), jnp.float32, 0.0, 1.0)
    loud = 2.0 ** jax.random.uniform(jax.random.fold_in(kz, 1), (), jnp.float32, -1.0, 2.0)
    layers = 2.0 ** jax.random.uniform(kl, (LAYERS, 1, 1), jnp.float32, -1.0, 1.0)
    x = together(ka, jax.random.normal(kx, shape, jnp.float32), much_x) * bump(kf, D, 4.0)
    dy = together(kb, jax.random.normal(kdy, shape, jnp.float32), much_dy)
    drawn = {"x": x.astype(jnp.bfloat16), "dy": (loud * dy * (SEQUENCES * TOKENS) ** -0.5).astype(jnp.bfloat16)}
    for key, name in zip(kw, NAMES, strict=True):
        w = jax.random.normal(key, SHAPES[name], jnp.float32) * SHAPES[name][1] ** -0.5
        drawn[name] = (w * {"w_gate": 1.0, "w_up": bump(kh, FF, 4.0), "w_down": layers}[name]).astype(jnp.bfloat16)
    for key, name in zip(km, NAMES, strict=True):
        drawn[f"m_{name}"] = 0.1 * jax.random.normal(key, SHAPES[name], jnp.float32)
    for key, name in zip(kv, NAMES, strict=True):
        drawn[f"v_{name}"] = jax.random.uniform(key, SHAPES[name], jnp.float32, 0.005, 0.015)
    return drawn


def matmul(a, w):
    return jnp.dot(a, w, preferred_element_type=jnp.float32).astype(jnp.bfloat16)


def normed(h):
    wide = h.astype(jnp.float32)
    scale = lax.rsqrt(jnp.mean(wide**2, -1, keepdims=True) + 1e-6)
    return (wide * scale).astype(jnp.bfloat16)


def layer(h, w):
    a = normed(h)
    gate = jnp.dot(a, w["w_gate"], preferred_element_type=jnp.float32)
    up = jnp.dot(a, w["w_up"], preferred_element_type=jnp.float32)
    return h + matmul((jax.nn.silu(gate) * up).astype(jnp.bfloat16), w["w_down"])


def adamw(w, m, v, g):
    m = 0.9 * m + 0.1 * g
    v = 0.95 * v + 0.05 * g * g
    step = m * lax.rsqrt(v + 1e-8) + 0.1 * w
    return (w - 0.02 * step).astype(jnp.bfloat16), m, v


def stack(weights, h):
    return lax.scan(lambda h, w: (layer(h, w), None), h, weights)[0]


def reference(x, dy, w_gate, w_up, w_down, m_w_gate, m_w_up, m_w_down, v_w_gate, v_w_up, v_w_down):
    weights = dict(zip(NAMES, (w_gate, w_up, w_down), strict=True))

    def take(so_far, sequence):
        h, by_y = sequence
        _, back = jax.vjp(lambda w: stack(w, h), weights)
        return jax.tree.map(lambda total, term: total + term.astype(jnp.float32), so_far, back(by_y)[0]), None

    none_yet = {name: jnp.zeros(w.shape, jnp.float32) for name, w in weights.items()}
    by_weights, _ = lax.scan(take, none_yet, (x, dy))
    gradients = [by_weights[name].astype(jnp.bfloat16).astype(jnp.float32) for name in NAMES]
    new = [
        adamw(w.astype(jnp.float32), m, v, g)
        for w, m, v, g in zip((w_gate, w_up, w_down), (m_w_gate, m_w_up, m_w_down), (v_w_gate, v_w_up, v_w_down), gradients, strict=True)
    ]
    return tuple(one[which] for which in range(3) for one in new)
```

```python
import itertools

import jax
import jax.numpy as jnp
from jax import lax
from jax.experimental import pallas as pl
from jax.experimental.pallas import tpu as pltpu
from jax.sharding import PartitionSpec as P

F32, BF16 = jnp.float32, jnp.bfloat16
T, D, FF = 2048, 1280, 4096
N = 16
TILE = 256
ROWS = D // N
ORDERS = ((0, 1, 2), (1, 2, 0), (2, 0, 1))


def params():
    return pltpu.CompilerParams(vmem_limit_bytes=64_000_000)


def cost(flops, nbytes):
    return pl.CostEstimate(flops=int(flops), bytes_accessed=int(nbytes), transcendentals=0)


def dot(a, b, ca, cb):
    return lax.dot_general(a, b, (((ca,), (cb,)), ((), ())), preferred_element_type=F32)


def shape(dims, dtype):
    return jax.ShapeDtypeStruct(dims, dtype)


def normed(wide):
    scale = lax.rsqrt(jnp.mean(wide**2, -1, keepdims=True) + 1e-6)
    return (wide * scale).astype(BF16)


def in_order(j, order):
    x, y, z = (j >> 2) & 1, (j >> 1) & 1, j & 1
    a, b, c = ((x, y, z)[axis] for axis in order)
    return (a << 2) | (b << 1) | c


def within(i, start, count):
    return jnp.clip(i - start, 0, count - 1)


def block_of(j, d, other):
    return ((j ^ (d >> 1)) << 1) | ((d & 1) ^ other)


PARTNERS = (1, 2, 4, 8)
IDS = itertools.count()


def ride(load, keep, came, out, sems, event):
    here = lax.axis_index("dp")
    local, sent, received = sems

    def exchange(p, k):
        bit = 1 if k == 0 else 8 >> ORDERS[p][k - 1]
        source = load[0][p] if k == 0 else keep[p].at[pl.ds(8 >> k, 8 >> k)]
        return pltpu.make_async_remote_copy(
            src_ref=source,
            dst_ref=came[p][k],
            send_sem=sent.at[4 * p + k],
            recv_sem=received.at[4 * p + k],
            device_id={"dp": here ^ bit},
            device_id_type=pl.DeviceIdType.MESH,
        )

    def own(p):
        return pltpu.make_async_copy(load[1][p], keep[p], local.at[p])

    if event == 0:
        for p in range(3):
            exchange(p, 0).start()
        for p in range(3):
            own(p).start()
        return
    for p in range(3):
        if event == 1:
            own(p).wait()
        exchange(p, event - 1).wait_recv()
    if event < 4:
        count = 8 >> event
        for p in range(3):

            @pl.loop(count, 2 * count)
            def _(b):
                total = keep[p][b].astype(F32)
                for k in range(event):
                    total = total + came[p][k][b].astype(F32)
                keep[p][b] = total.astype(BF16)

        for p in range(3):
            exchange(p, event).start()
        return
    at = 0
    for p in range(3):
        total = keep[p][0].astype(F32)
        for k in range(4):
            total = total + came[p][k][0].astype(F32)
        out[:, at : at + total.shape[1]] = total.astype(BF16)
        at += total.shape[1]
        for k in range(4):
            exchange(p, k).wait_send()


def call(body, steps, ins, outs, args, riders=(), scratch=(), flops=0, nbytes=0, aliases=None, name=None):
    n_in, n_out, n_scratch, n = len(ins), len(outs), len(scratch), len(riders)
    events = [0, max(1, round(0.2 * steps)), round(0.55 * steps), round(0.8 * steps)]

    def whole(*refs):
        refs = list(refs)

        def take(count):
            some = refs[:count]
            del refs[:count]
            return some

        own_in = take(n_in)
        loads = [(take(3), take(3)) for _ in riders]
        own_out = take(n_out)
        sums = take(n)
        own_scratch = take(n_scratch)
        rides = []
        for q in range(n):
            keep = take(3)
            came = [take(4) for _ in range(3)]
            rides.append((loads[q], keep, came, sums[q], take(3)))
        i = pl.program_id(0)
        if n:

            def go(event):
                if event == 0:
                    here = lax.axis_index("dp")
                    barrier = pltpu.get_barrier_semaphore()
                    for bit in PARTNERS:
                        pl.semaphore_signal(barrier, inc=1, device_id={"dp": here ^ bit}, device_id_type=pl.DeviceIdType.MESH)
                    pl.semaphore_wait(barrier, len(PARTNERS))
                for one in rides:
                    ride(*one, event)

            for event in range(4):
                if steps == 1:
                    go(event)
                else:
                    pl.when(i == events[event])(lambda event=event: go(event))

        if body is not None:
            body(*own_in, *own_out, *own_scratch)

        if n:
            if steps == 1:
                go(4)
            else:
                pl.when(i == steps - 1)(lambda: go(4))

    ride_scratch, sum_outs, extra = [], [], {}
    for send, keep in riders:
        rows = keep[0].shape[1]
        ride_scratch += [pltpu.VMEM(t.shape, BF16) for t in keep]
        for t in keep:
            ride_scratch += [pltpu.VMEM((count, *t.shape[1:]), BF16) for count in (8, 4, 2, 1)]
        ride_scratch += [pltpu.SemaphoreType.DMA((3,)), pltpu.SemaphoreType.DMA((12,)), pltpu.SemaphoreType.DMA((12,))]
        form = (rows, sum(t.shape[2] for t in keep))
        sum_outs.append((pl.BlockSpec(form, lambda i: (0, 0)), shape(form, BF16)))
        extra = {"has_side_effects": True}
    if riders:
        extra["collective_id"] = next(IDS)
    outs = list(outs) + sum_outs
    result = pl.pallas_call(
        whole,
        grid=(steps,),
        in_specs=list(ins) + [pl.BlockSpec(memory_space=pl.ANY)] * (6 * n),
        out_specs=[spec for spec, _ in outs],
        out_shape=[form for _, form in outs],
        scratch_shapes=list(scratch) + ride_scratch,
        input_output_aliases=aliases or {},
        compiler_params=pltpu.CompilerParams(vmem_limit_bytes=66_000_000, **extra),
        cost_estimate=cost(flops, nbytes),
        name=name,
    )(*args, *[t for send, keep in riders for t in (*send, *keep)])
    return list(result[:n_out]), list(result[n_out:])


def forward(a, w_gate, w_up, number):
    def body(a, wg, wu, act, gate, up):
        g = dot(a[...], wg[...], 1, 0)
        u = dot(a[...], wu[...], 1, 0)
        gate[...] = g
        up[...] = u
        act[...] = (jax.nn.silu(g) * u).astype(BF16)

    tile = pl.BlockSpec((T, TILE), lambda j: (0, j))
    w = pl.BlockSpec((None, D, TILE), lambda j: (number, 0, j))
    return pl.pallas_call(
        body,
        grid=(FF // TILE,),
        in_specs=[pl.BlockSpec((T, D), lambda j: (0, 0)), w, w],
        out_specs=[tile] * 3,
        out_shape=[shape((T, FF), BF16), shape((T, FF), F32), shape((T, FF), F32)],
        compiler_params=params(),
        cost_estimate=cost(4 * T * D * FF, 140e6),
        name="forward",
    )(a, w_gate, w_up)


def prepare(x):
    rows = 256

    def body(x, a, at):
        new = normed(x[...].astype(F32))
        a[...] = new
        at[...] = new.T

    some = pl.BlockSpec((rows, D), lambda i: (i, 0))
    return pl.pallas_call(
        body,
        grid=(T // rows,),
        in_specs=[some],
        out_specs=[some, pl.BlockSpec((D, rows), lambda i: (0, i))],
        out_shape=[shape((T, D), BF16), shape((D, T), BF16)],
        compiler_params=params(),
        cost_estimate=cost(1e8, 16e6),
        name="prepare",
    )(x)


def down(act, h, w_down, number):
    rows = 256

    def body(act, h, w, out, a, at):
        new = h[...] + dot(act[...], w[...], 1, 0).astype(BF16)
        out[...] = new
        new = normed(new.astype(F32))
        a[...] = new
        at[...] = new.T

    some = pl.BlockSpec((rows, D), lambda i: (i, 0))
    return pl.pallas_call(
        body,
        grid=(T // rows,),
        in_specs=[
            pl.BlockSpec((rows, FF), lambda i: (i, 0)),
            some,
            pl.BlockSpec((None, FF, D), lambda i: (number, 0, 0), pipeline_mode=pl.Buffered(1)),
        ],
        out_specs=[some, some, pl.BlockSpec((D, rows), lambda i: (0, i))],
        out_shape=[shape((T, D), BF16)] * 2 + [shape((D, T), BF16)],
        compiler_params=params(),
        cost_estimate=cost(2 * T * D * FF, 40e6),
        name="down",
    )(act, h, w_down)


def gradients_in(at, rows, held, outs, sems, tiles, parts):
    half = N // 2
    i = pl.program_id(0)
    here = lax.axis_index("dp")
    starts = [sum(parts[:p]) for p in range(3)]
    loads = [
        pltpu.make_async_copy(
            at.at[block_of(j & 7, here, 1 - (j >> 3))], rows.at[pl.ds(j * ROWS, ROWS)], sems[0].at[j]
        )
        for j in range(N)
    ]
    each = tiles // (len(held) // 6)
    puts = [pltpu.make_async_copy(held[k], outs[k], sems[1].at[k]) for k in range(len(held))]

    def begin():
        @pl.when(i == 0)
        def _():
            for load in loads:
                load.start()

    def finish(by_gate, by_up):
        @pl.when(i == 0)
        def _():
            for load in loads:
                load.wait()

        both = dot(rows[...], jnp.concatenate([by_gate, by_up], axis=1), 1, 0).astype(BF16)
        for step in range(tiles):

            @pl.when(i == step)
            def _():
                unit = step // each
                for which in range(2):
                    t = which * each + step % each
                    p = max(q for q in range(3) if starts[q] <= t)
                    columns = slice((t - starts[p]) * TILE, (t - starts[p] + 1) * TILE)
                    new = both[:, which * TILE : (which + 1) * TILE]
                    for k in range(2):
                        for j in range(half):
                            row = (k * half + j) * ROWS
                            held[6 * unit + 3 * k + p][in_order(j, ORDERS[p]), :, columns] = new[row : row + ROWS]
                if (step + 1) % each == 0:
                    for put in puts[6 * unit : 6 * unit + 6]:
                        put.start()

        @pl.when(i == tiles - 1)
        def _():
            for put in puts:
                put.wait()

    return begin, finish


def gradient_forms(units, parts):
    half = N // 2
    forms = [(half, ROWS, parts[p] * TILE) for unit in range(units) for k in range(2) for p in range(3)]
    outs = [(pl.BlockSpec(memory_space=pl.ANY), shape(form, BF16)) for form in forms]
    scratch = [pltpu.VMEM((D, T), BF16)] + [pltpu.VMEM(form, BF16) for form in forms]
    return outs, scratch + [pltpu.SemaphoreType.DMA((N,)), pltpu.SemaphoreType.DMA((6 * units,))]


def back(g, u, c):
    c = c.astype(BF16).astype(F32)
    sig = jax.nn.sigmoid(g)
    silu = g * sig
    return (silu * u).astype(BF16), (c * u * (sig * (1 + g * (1 - sig)))).astype(BF16), (c * silu).astype(BF16)


def last_layer(riders, a, at, dy, w_gate, w_up, w_down, number, first, tiles, parts, so_far):
    n = len(so_far)

    def body(a, dy, wg, wu, wd, at, *refs):
        refs = refs[n:]
        dgate, dup, act = refs[:3]
        outs, (rows, *held, loaded, put) = refs[3:9], refs[9:]
        begin, finish = gradients_in(at, rows, held, outs, (loaded, put), tiles, parts)
        begin()
        g = dot(a[...], wg[...], 1, 0)
        u = dot(a[...], wu[...], 1, 0)
        act[...], dgate[...], dup[...] = back(g, u, dot(dy[...], wd[...], 1, 1))
        finish(dgate[...], dup[...])

    full = pl.BlockSpec((T, D), lambda j: (0, 0), pipeline_mode=pl.Buffered(1))
    tile = pl.BlockSpec((T, TILE), lambda j: (0, first + j))
    w = pl.BlockSpec((None, D, TILE), lambda j: (number, 0, first + j))
    wd = pl.BlockSpec((None, TILE, D), lambda j: (number, first + j, 0))
    anywhere = pl.BlockSpec(memory_space=pl.ANY)
    outs, scratch = gradient_forms(1, parts)
    outs, sums = call(
        body,
        tiles,
        [full, full, w, w, wd, anywhere] + [anywhere] * n,
        [(tile, shape((T, FF), BF16))] * 3 + outs,
        (a, dy, w_gate, w_up, w_down, at, *so_far),
        riders,
        scratch=scratch,
        aliases={6: 0, 7: 1, 8: 2} if so_far else {},
        flops=10 * T * D * TILE * tiles,
        nbytes=8e6 * tiles,
        name="last_layer",
    )
    return (outs[:3], (outs[3:6], outs[6:])), sums


def first_layer(riders, dh, at, gate, up, w_down, number, first, units, parts):
    tiles = units * TILES

    def body(dh, g, u, wd, at, *refs):
        outs, (rows, *held, loaded, put) = refs[: 6 * units], refs[6 * units :]
        begin, finish = gradients_in(at, rows, held, outs, (loaded, put), tiles, parts)
        begin()
        _, dgate, dup = back(g[...], u[...], dot(dh[...], wd[...], 1, 1))
        finish(dgate, dup)

    full = pl.BlockSpec((T, D), lambda j: (0, 0), pipeline_mode=pl.Buffered(1))
    kept = pl.BlockSpec((T, TILE), lambda j: (0, first + j))
    wd = pl.BlockSpec((None, TILE, D), lambda j: (number, first + j, 0))
    outs, scratch = gradient_forms(units, parts)
    outs, sums = call(
        body,
        tiles,
        [full, kept, kept, wd, pl.BlockSpec(memory_space=pl.ANY)],
        outs,
        (dh, gate, up, w_down, at),
        riders,
        scratch=scratch,
        flops=6 * T * D * TILE * tiles,
        nbytes=8e6 * tiles,
        name="first_layer",
    )
    return [(outs[k : k + 3], outs[k + 3 : k + 6]) for k in range(0, 6 * units, 6)], sums


def gradient_out(riders, act, dy, parts):
    half = N // 2
    starts = [128 * sum(parts[:p]) for p in range(3)]
    rows = TILE // 2

    def body(act, dy, *outs):
        new = dot(act[...], dy[...], 0, 0).astype(BF16)
        for k in range(2):

            @pl.when((pl.program_id(0) >> 3) == k)
            def _():
                for q in range(2):
                    for p in range(3):
                        columns = slice(starts[p], starts[p] + 128 * parts[p])
                        outs[6 * q + 3 * k + p][...] = new[q * rows : (q + 1) * rows, columns]

    def out_spec(k, p):
        return pl.BlockSpec((None, rows, 128 * parts[p]), lambda i: (in_order(within(i, k * half, half), ORDERS[p]), 0, 0))

    outs, sums = call(
        body,
        N,
        [
            pl.BlockSpec((T, TILE), lambda i: (0, block_of(i & 7, lax.axis_index("dp"), 1 - (i >> 3)))),
            pl.BlockSpec((T, D), lambda i: (0, 0), pipeline_mode=pl.Buffered(1)),
        ],
        [(out_spec(k, p), shape((half, rows, 128 * parts[p]), BF16)) for q in range(2) for k in range(2) for p in range(3)],
        (act, dy),
        riders,
        flops=2 * T * D * FF,
        nbytes=33e6,
        name="gradient_out",
    )
    return [(outs[:3], outs[3:6]), (outs[6:9], outs[9:])], sums


def states_backward(riders, dgate, dup, w_gate, w_up, h, dy, number):
    wide = 512

    def body(dg, du, wg, wu, h, dy, out, by_gate, by_up, states, sem):
        i = pl.program_id(0)
        load = pltpu.make_async_copy(h, states, sem.at[0])
        put = pltpu.make_async_copy(states, out, sem.at[1])

        @pl.when(i == 0)
        def _():
            load.start()
            by_gate[...] = dot(dg[...], wg[...], 1, 1)
            by_up[...] = dot(du[...], wu[...], 1, 1)

        @pl.when(i > 0)
        def _():
            by_gate[...] += dot(dg[...], wg[...], 1, 1)
            by_up[...] += dot(du[...], wu[...], 1, 1)

        @pl.when(i == FF // wide - 1)
        def _():
            rows = 256
            load.wait()

            @pl.loop(0, T // rows)
            def _(r):
                at = pl.ds(pl.multiple_of(r * rows, rows), rows)
                da = (by_gate[at, :].astype(BF16) + by_up[at, :].astype(BF16)).astype(F32)
                x = states[at, :].astype(F32)
                scale = lax.rsqrt(jnp.mean(x**2, -1, keepdims=True) + 1e-6)
                along = jnp.mean(da * x, -1, keepdims=True)
                dx = da * scale - x * (scale**3 * along)
                states[at, :] = dy[at, :] + dx.astype(BF16)

            put.start()
            put.wait()

    full = pl.BlockSpec((T, D), lambda i: (0, 0), pipeline_mode=pl.Buffered(1))
    anywhere = pl.BlockSpec(memory_space=pl.ANY)
    tile = pl.BlockSpec((T, wide), lambda i: (0, i))
    w = pl.BlockSpec((None, D, wide), lambda i: (number, 0, i))
    (out,), sums = call(
        body,
        FF // wide,
        [tile, tile, w, w, anywhere, full],
        [(anywhere, shape((T, D), BF16))],
        (dgate, dup, w_gate, w_up, h, dy),
        riders,
        scratch=[pltpu.VMEM((T, D), F32)] * 2 + [pltpu.VMEM((T, D), BF16), pltpu.SemaphoreType.DMA((2,))],
        flops=4 * T * D * FF,
        nbytes=70e6,
        name="states_backward",
    )
    return out, sums


def update_in(place, sums, w_gate, w_up, m, v, number, first, tiles):
    steps, wide = 5, tiles * TILE
    rows, n = ROWS // steps, len(sums)

    def body(s, *refs):
        new, at = refs[-1], 0
        for q in range(n):
            for k in range(2):
                w, m, v = refs[n + 3 * (2 * q + k) :][:3]
                g = refs[q][:, k * wide : (k + 1) * wide]
                new[:, at : at + wide] = new_weight(w[...], m[...], v[...], g)
                at += wide

    def state(q):
        return pl.BlockSpec((None, rows, wide), lambda i, s: (number, i, first // tiles + q))

    def own(q):
        return pl.BlockSpec((None, rows, wide), lambda i, s: (number, s[0] * steps + i, first // tiles + q))

    return pl.pallas_call(
        body,
        grid_spec=pltpu.PrefetchScalarGridSpec(
            num_scalar_prefetch=1,
            grid=(steps,),
            in_specs=[pl.BlockSpec((rows, 2 * wide), lambda i, s: (i, 0))] * n
            + [spec for q in range(n) for _ in range(2) for spec in (own(q), state(q), state(q))],
            out_specs=pl.BlockSpec((rows, 2 * n * wide), lambda i, s: (i, 0)),
        ),
        out_shape=shape((ROWS, 2 * n * wide), BF16),
        compiler_params=params(),
        cost_estimate=cost(1e8, 1e7),
        name="update_in",
    )(place, *sums, *[t for q in range(n) for one in zip((w_gate, w_up), m, v) for t in one])


def update_out(place, sums, w_down, m, v, number):
    rows = TILE // 2

    def body(s, one, two, w, m, v, new):
        for q, g in enumerate((one, two)):

            @pl.when(pl.program_id(0) == q)
            def _():
                new[...] = new_weight(w[...], m[...], v[...], g[...])

    whole = pl.BlockSpec((rows, D), lambda i, s: (0, 0))
    state = pl.BlockSpec((None, rows, D), lambda i, s: (number, i, 0))
    own = pl.BlockSpec((None, rows, D), lambda i, s: (number, s[0] * 2 + i, 0))
    return pl.pallas_call(
        body,
        grid_spec=pltpu.PrefetchScalarGridSpec(
            num_scalar_prefetch=1,
            grid=(2,),
            in_specs=[whole, whole, own, state, state],
            out_specs=pl.BlockSpec((rows, D), lambda i, s: (i, 0)),
        ),
        out_shape=shape((TILE, D), BF16),
        compiler_params=params(),
        cost_estimate=cost(1e8, 1e7),
        name="update_out",
    )(place, *sums, w_down, m, v)


def lay_in(gathered, outs, number, first, tiles):
    wide, rows = 512, 640
    each = tiles * TILE // wide
    blocks = gathered.shape[1] // 2 // wide

    def body(gate, up, *refs):
        refs[-2][...] = gate[...]
        refs[-1][...] = up[...]

    out = pl.BlockSpec((None, rows, wide), lambda i, j: (number, i, first * TILE // wide + j))
    return pl.pallas_call(
        body,
        grid=(D // rows, blocks),
        in_specs=[
            pl.BlockSpec((rows, wide), lambda i, j: (i, (j // each) * 2 * each + j % each)),
            pl.BlockSpec((rows, wide), lambda i, j: (i, (j // each) * 2 * each + each + j % each)),
        ]
        + [pl.BlockSpec(memory_space=pl.ANY)] * len(outs),
        out_specs=[out, out],
        out_shape=[shape((2, D, FF), BF16)] * 2,
        input_output_aliases={2: 0, 3: 1} if outs else {},
        compiler_params=params(),
        cost_estimate=cost(1e8, 2e7),
        name="lay_in",
    )(gathered, gathered, *outs)


def lay_out(gathered, outs, number):
    rows = 512

    def body(new, *refs):
        refs[-1][...] = new[...]

    return pl.pallas_call(
        body,
        grid=(FF // rows,),
        in_specs=[pl.BlockSpec((rows, D), lambda i: (i, 0))] + [pl.BlockSpec(memory_space=pl.ANY)] * len(outs),
        out_specs=[pl.BlockSpec((None, rows, D), lambda i: (number, i, 0))],
        out_shape=[shape((2, FF, D), BF16)],
        input_output_aliases={1: 0} if outs else {},
        compiler_params=params(),
        cost_estimate=cost(1e8, 4 * D * FF),
        name="lay_out",
    )(gathered, *outs)


def moments(m, v, g):
    g = g.astype(F32)
    return 0.9 * m + 0.1 * g, 0.95 * v + 0.05 * g * g


def new_weight(w, m, v, g):
    m, v = moments(m, v, g)
    step = m * lax.rsqrt(v + 1e-8) + 0.1 * w.astype(F32)
    return (w.astype(F32) - 0.02 * step).astype(BF16)


class Line:
    def __init__(self):
        self.last = ()

    def run(self, f, first, *rest):
        first, self.last = lax.optimization_barrier((first, self.last))
        out = f(first, *rest)
        self.last = jax.tree.leaves(out)[-1:]
        return out


TILES = 4
PARTS = (3, 3, 2)
PARTS_OUT = ((4, 3, 3), (3, 4, 3))
UNITS = (2, 1, 1)
GROUPS = ((2, 1, 1), (2, 2))


def solution(mesh):
    def step(x, dy, w_gate, w_up, w_down, *state):
        m, v = state[:3], state[3:]
        x, dy = x[0], dy[0]
        place = lax.axis_index("dp").astype(jnp.int32).reshape(1)
        line = Line()
        queue, done, lays = [], {}, []
        outs = {"in": [], "out": []}
        groups = [(number, "out", (0, 1)) for number in (0, 1)]
        for number in (0, 1):
            first = 0
            for size in GROUPS[number]:
                groups.append((number, "in", tuple(range(first, first + size))))
                first += size

        def gather(number, kind, members):
            sums = [done[number, kind, one] for one in members]
            if kind == "in":
                first = members[0] * TILES
                new = line.run(update_in, place, sums, w_gate, w_up, m[:2], v[:2], number, first, TILES)
            else:
                new = line.run(update_out, place, sums, w_down, m[2], v[2], number)
            new = lax.all_gather(new, "dp", axis=0, tiled=True)

            def lay():
                if kind == "in":
                    outs["in"] = line.run(lay_in, new, outs["in"], number, first, TILES)
                else:
                    outs["out"] = line.run(lay_out, new, outs["out"], number)

            lays.append(lay)

        def run(room, f, *args):
            riding = queue[:room]
            del queue[:room]

            def beside(both, *rest):
                return f(both[0], *both[1], *rest)

            out, sums = line.run(beside, ([halves for _, halves in riding], args[:1]), *args[1:])
            for (name, _), one in zip(riding, sums):
                done[name] = one
            for group in list(groups):
                number, kind, members = group
                if all((number, kind, one) in done for one in members):
                    groups.remove(group)
                    gather(*group)
            return out

        def only(riders, _):
            return call(None, 1, [], [], (), riders, name="exchange")

        a0, at0 = line.run(prepare, x)
        act0, gate0, up0 = line.run(forward, a0, w_gate, w_up, 0)
        h1, a1, at1 = line.run(down, act0, x, w_down, 0)
        at0, at1 = (t.reshape(N, ROWS, T) for t in (at0, at1))

        so_far = []
        for k in range(N // TILES):
            so_far, halves = run(1, last_layer, a1, at1, dy, w_gate, w_up, w_down, 1, k * TILES, TILES, PARTS, so_far)
            queue.append(((1, "in", k), halves))
        dgate, dup, act1 = so_far
        for k, halves in enumerate(run(1, gradient_out, act1, dy, PARTS_OUT[1])):
            queue.append(((1, "out", k), halves))
        dh1 = run(1, states_backward, dgate, dup, w_gate, w_up, h1, dy, 1)
        for k, halves in enumerate(run(1, gradient_out, act0, dh1, PARTS_OUT[0])):
            queue.append(((0, "out", k), halves))
        k = 0
        for units in UNITS:
            for halves in run(2, first_layer, dh1, at0, gate0, up0, w_down, 0, k * TILES, units, PARTS):
                queue.append(((0, "in", k), halves))
                k += 1
        while queue:
            run(2, only, place)
        for lay in lays:
            lay()

        new_m, new_v = [], []
        for k in range(3):
            layers = []
            for number in range(2):
                if k == 2:
                    layers.append(jnp.concatenate([done[number, "out", q] for q in range(2)], axis=0))
                else:
                    columns = slice(k * TILES * TILE, (k + 1) * TILES * TILE)
                    layers.append(
                        jnp.concatenate([done[number, "in", q][:, columns] for q in range(N // TILES)], axis=1)
                    )
            one_m, one_v = moments(m[k], v[k], jnp.stack(layers))
            new_m.append(one_m)
            new_v.append(one_v)
        return (*outs["in"], *outs["out"], *new_m, *new_v)

    rows = P(None, "dp", None)
    return jax.shard_map(
        step,
        mesh=mesh,
        in_specs=(P(("rep", "dp")),) * 2 + (P(),) * 3 + (rows,) * 6,
        out_specs=(P("rep"),) * 3 + (P("rep", "dp", None),) * 6,
        check_vma=False,
    )
```

```python
import itertools

import jax
import jax.numpy as jnp
from jax import lax
from jax.experimental import pallas as pl
from jax.experimental.pallas import tpu as pltpu
from jax.sharding import PartitionSpec as P

F32, BF16 = jnp.float32, jnp.bfloat16
T, D, FF = 2048, 1280, 4096
N = 16
TILE = 256
ROWS = D // N
ORDERS = ((0, 1, 2), (1, 2, 0), (2, 0, 1))


def params():
    return pltpu.CompilerParams(vmem_limit_bytes=64_000_000)


def cost(flops, nbytes):
    return pl.CostEstimate(flops=int(flops), bytes_accessed=int(nbytes), transcendentals=0)


def dot(a, b, ca, cb):
    return lax.dot_general(a, b, (((ca,), (cb,)), ((), ())), preferred_element_type=F32)


def shape(dims, dtype):
    return jax.ShapeDtypeStruct(dims, dtype)


def normed(wide):
    scale = lax.rsqrt(jnp.mean(wide**2, -1, keepdims=True) + 1e-6)
    return (wide * scale).astype(BF16)


def in_order(j, order):
    x, y, z = (j >> 2) & 1, (j >> 1) & 1, j & 1
    a, b, c = ((x, y, z)[axis] for axis in order)
    return (a << 2) | (b << 1) | c


def within(i, start, count):
    return jnp.clip(i - start, 0, count - 1)


def block_of(j, d, other):
    return ((j ^ (d >> 1)) << 1) | ((d & 1) ^ other)


PARTNERS = (1, 2, 4, 8)
IDS = itertools.count()


def ride(load, keep, came, out, sems, event):
    here = lax.axis_index("dp")
    local, sent, received = sems

    def exchange(p, k):
        bit = 1 if k == 0 else 8 >> ORDERS[p][k - 1]
        source = load[0][p] if k == 0 else keep[p].at[pl.ds(8 >> k, 8 >> k)]
        return pltpu.make_async_remote_copy(
            src_ref=source,
            dst_ref=came[p][k],
            send_sem=sent.at[4 * p + k],
            recv_sem=received.at[4 * p + k],
            device_id={"dp": here ^ bit},
            device_id_type=pl.DeviceIdType.MESH,
        )

    def own(p):
        return pltpu.make_async_copy(load[1][p], keep[p], local.at[p])

    if event == 0:
        for p in range(3):
            exchange(p, 0).start()
        for p in range(3):
            own(p).start()
        return
    for p in range(3):
        if event == 1:
            own(p).wait()
        exchange(p, event - 1).wait_recv()
    if event < 4:
        count = 8 >> event
        for p in range(3):

            @pl.loop(count, 2 * count)
            def _(b):
                total = keep[p][b].astype(F32)
                for k in range(event):
                    total = total + came[p][k][b].astype(F32)
                keep[p][b] = total.astype(BF16)

        for p in range(3):
            exchange(p, event).start()
        return
    at = 0
    for p in range(3):
        total = keep[p][0].astype(F32)
        for k in range(4):
            total = total + came[p][k][0].astype(F32)
        out[:, at : at + total.shape[1]] = total.astype(BF16)
        at += total.shape[1]
        for k in range(4):
            exchange(p, k).wait_send()


def call(body, steps, ins, outs, args, riders=(), scratch=(), flops=0, nbytes=0, aliases=None, name=None):
    n_in, n_out, n_scratch, n = len(ins), len(outs), len(scratch), len(riders)
    events = [0, max(1, round(0.2 * steps)), round(0.55 * steps), round(0.8 * steps)]

    def whole(*refs):
        refs = list(refs)

        def take(count):
            some = refs[:count]
            del refs[:count]
            return some

        own_in = take(n_in)
        loads = [(take(3), take(3)) for _ in riders]
        own_out = take(n_out)
        sums = take(n)
        own_scratch = take(n_scratch)
        rides = []
        for q in range(n):
            keep = take(3)
            came = [take(4) for _ in range(3)]
            rides.append((loads[q], keep, came, sums[q], take(3)))
        i = pl.program_id(0)
        if n:

            def go(event):
                if event == 0:
                    here = lax.axis_index("dp")
                    barrier = pltpu.get_barrier_semaphore()
                    for bit in PARTNERS:
                        pl.semaphore_signal(barrier, inc=1, device_id={"dp": here ^ bit}, device_id_type=pl.DeviceIdType.MESH)
                    pl.semaphore_wait(barrier, len(PARTNERS))
                for one in rides:
                    ride(*one, event)

            for event in range(4):
                if steps == 1:
                    go(event)
                else:
                    pl.when(i == events[event])(lambda event=event: go(event))

        if body is not None:
            body(*own_in, *own_out, *own_scratch)

        if n:
            if steps == 1:
                go(4)
            else:
                pl.when(i == steps - 1)(lambda: go(4))

    ride_scratch, sum_outs, extra = [], [], {}
    for send, keep in riders:
        rows = keep[0].shape[1]
        ride_scratch += [pltpu.VMEM(t.shape, BF16) for t in keep]
        for t in keep:
            ride_scratch += [pltpu.VMEM((count, *t.shape[1:]), BF16) for count in (8, 4, 2, 1)]
        ride_scratch += [pltpu.SemaphoreType.DMA((3,)), pltpu.SemaphoreType.DMA((12,)), pltpu.SemaphoreType.DMA((12,))]
        form = (rows, sum(t.shape[2] for t in keep))
        sum_outs.append((pl.BlockSpec(form, lambda i: (0, 0)), shape(form, BF16)))
        extra = {"has_side_effects": True}
    if riders:
        extra["collective_id"] = next(IDS)
    outs = list(outs) + sum_outs
    result = pl.pallas_call(
        whole,
        grid=(steps,),
        in_specs=list(ins) + [pl.BlockSpec(memory_space=pl.ANY)] * (6 * n),
        out_specs=[spec for spec, _ in outs],
        out_shape=[form for _, form in outs],
        scratch_shapes=list(scratch) + ride_scratch,
        input_output_aliases=aliases or {},
        compiler_params=pltpu.CompilerParams(vmem_limit_bytes=66_000_000, **extra),
        cost_estimate=cost(flops, nbytes),
        name=name,
    )(*args, *[t for send, keep in riders for t in (*send, *keep)])
    return list(result[:n_out]), list(result[n_out:])


def forward(a, w_gate, w_up, number):
    def body(a, wg, wu, act, gate, up):
        g = dot(a[...], wg[...], 1, 0)
        u = dot(a[...], wu[...], 1, 0)
        gate[...] = g
        up[...] = u
        act[...] = (jax.nn.silu(g) * u).astype(BF16)

    tile = pl.BlockSpec((T, TILE), lambda j: (0, j))
    w = pl.BlockSpec((None, D, TILE), lambda j: (number, 0, j))
    return pl.pallas_call(
        body,
        grid=(FF // TILE,),
        in_specs=[pl.BlockSpec((T, D), lambda j: (0, 0)), w, w],
        out_specs=[tile] * 3,
        out_shape=[shape((T, FF), BF16), shape((T, FF), F32), shape((T, FF), F32)],
        compiler_params=params(),
        cost_estimate=cost(4 * T * D * FF, 140e6),
        name="forward",
    )(a, w_gate, w_up)


def prepare(x):
    rows = 256

    def body(x, a, at):
        new = normed(x[...].astype(F32))
        a[...] = new
        at[...] = new.T

    some = pl.BlockSpec((rows, D), lambda i: (i, 0))
    return pl.pallas_call(
        body,
        grid=(T // rows,),
        in_specs=[some],
        out_specs=[some, pl.BlockSpec((D, rows), lambda i: (0, i))],
        out_shape=[shape((T, D), BF16), shape((D, T), BF16)],
        compiler_params=params(),
        cost_estimate=cost(1e8, 16e6),
        name="prepare",
    )(x)


def down(act, h, w_down, number):
    rows = 256

    def body(act, h, w, out, a, at):
        new = h[...] + dot(act[...], w[...], 1, 0).astype(BF16)
        out[...] = new
        new = normed(new.astype(F32))
        a[...] = new
        at[...] = new.T

    some = pl.BlockSpec((rows, D), lambda i: (i, 0))
    return pl.pallas_call(
        body,
        grid=(T // rows,),
        in_specs=[
            pl.BlockSpec((rows, FF), lambda i: (i, 0)),
            some,
            pl.BlockSpec((None, FF, D), lambda i: (number, 0, 0), pipeline_mode=pl.Buffered(1)),
        ],
        out_specs=[some, some, pl.BlockSpec((D, rows), lambda i: (0, i))],
        out_shape=[shape((T, D), BF16)] * 2 + [shape((D, T), BF16)],
        compiler_params=params(),
        cost_estimate=cost(2 * T * D * FF, 40e6),
        name="down",
    )(act, h, w_down)


def gradients_in(at, rows, held, outs, sems, tiles, parts):
    half = N // 2
    i = pl.program_id(0)
    here = lax.axis_index("dp")
    starts = [sum(parts[:p]) for p in range(3)]
    loads = [
        pltpu.make_async_copy(
            at.at[block_of(j & 7, here, 1 - (j >> 3))], rows.at[pl.ds(j * ROWS, ROWS)], sems[0].at[j]
        )
        for j in range(N)
    ]
    each = tiles // (len(held) // 6)
    puts = [pltpu.make_async_copy(held[k], outs[k], sems[1].at[k]) for k in range(len(held))]

    def begin():
        @pl.when(i == 0)
        def _():
            for load in loads:
                load.start()

    def finish(by_gate, by_up):
        @pl.when(i == 0)
        def _():
            for load in loads:
                load.wait()

        both = dot(rows[...], jnp.concatenate([by_gate, by_up], axis=1), 1, 0).astype(BF16)
        for step in range(tiles):

            @pl.when(i == step)
            def _():
                unit = step // each
                for which in range(2):
                    t = which * each + step % each
                    p = max(q for q in range(3) if starts[q] <= t)
                    columns = slice((t - starts[p]) * TILE, (t - starts[p] + 1) * TILE)
                    new = both[:, which * TILE : (which + 1) * TILE]
                    for k in range(2):
                        for j in range(half):
                            row = (k * half + j) * ROWS
                            held[6 * unit + 3 * k + p][in_order(j, ORDERS[p]), :, columns] = new[row : row + ROWS]
                if (step + 1) % each == 0:
                    for put in puts[6 * unit : 6 * unit + 6]:
                        put.start()

        @pl.when(i == tiles - 1)
        def _():
            for put in puts:
                put.wait()

    return begin, finish


def gradient_forms(units, parts):
    half = N // 2
    forms = [(half, ROWS, parts[p] * TILE) for unit in range(units) for k in range(2) for p in range(3)]
    outs = [(pl.BlockSpec(memory_space=pl.ANY), shape(form, BF16)) for form in forms]
    scratch = [pltpu.VMEM((D, T), BF16)] + [pltpu.VMEM(form, BF16) for form in forms]
    return outs, scratch + [pltpu.SemaphoreType.DMA((N,)), pltpu.SemaphoreType.DMA((6 * units,))]


def back(g, u, c):
    c = c.astype(BF16).astype(F32)
    sig = jax.nn.sigmoid(g)
    silu = g * sig
    return (silu * u).astype(BF16), (c * u * (sig * (1 + g * (1 - sig)))).astype(BF16), (c * silu).astype(BF16)


def last_layer(riders, a, at, dy, w_gate, w_up, w_down, number, first, tiles, parts, so_far):
    n = len(so_far)

    def body(a, dy, wg, wu, wd, at, *refs):
        refs = refs[n:]
        dgate, dup, act = refs[:3]
        outs, (rows, *held, loaded, put) = refs[3:9], refs[9:]
        begin, finish = gradients_in(at, rows, held, outs, (loaded, put), tiles, parts)
        begin()
        g = dot(a[...], wg[...], 1, 0)
        u = dot(a[...], wu[...], 1, 0)
        act[...], dgate[...], dup[...] = back(g, u, dot(dy[...], wd[...], 1, 1))
        finish(dgate[...], dup[...])

    full = pl.BlockSpec((T, D), lambda j: (0, 0), pipeline_mode=pl.Buffered(1))
    tile = pl.BlockSpec((T, TILE), lambda j: (0, first + j))
    w = pl.BlockSpec((None, D, TILE), lambda j: (number, 0, first + j))
    wd = pl.BlockSpec((None, TILE, D), lambda j: (number, first + j, 0))
    anywhere = pl.BlockSpec(memory_space=pl.ANY)
    outs, scratch = gradient_forms(1, parts)
    outs, sums = call(
        body,
        tiles,
        [full, full, w, w, wd, anywhere] + [anywhere] * n,
        [(tile, shape((T, FF), BF16))] * 3 + outs,
        (a, dy, w_gate, w_up, w_down, at, *so_far),
        riders,
        scratch=scratch,
        aliases={6: 0, 7: 1, 8: 2} if so_far else {},
        flops=10 * T * D * TILE * tiles,
        nbytes=8e6 * tiles,
        name="last_layer",
    )
    return (outs[:3], (outs[3:6], outs[6:])), sums


def first_layer(riders, dh, at, gate, up, w_down, number, first, units, parts):
    tiles = units * TILES

    def body(dh, g, u, wd, at, *refs):
        outs, (rows, *held, loaded, put) = refs[: 6 * units], refs[6 * units :]
        begin, finish = gradients_in(at, rows, held, outs, (loaded, put), tiles, parts)
        begin()
        some = [pl.ds(r * 512, 512) for r in range(T // 512)]
        rows_of = [back(g[at, :], u[at, :], dot(dh[at, :], wd[...], 1, 1)) for at in some]
        finish(jnp.concatenate([one[1] for one in rows_of]), jnp.concatenate([one[2] for one in rows_of]))

    full = pl.BlockSpec((T, D), lambda j: (0, 0), pipeline_mode=pl.Buffered(1))
    kept = pl.BlockSpec((T, TILE), lambda j: (0, first + j))
    wd = pl.BlockSpec((None, TILE, D), lambda j: (number, first + j, 0))
    outs, scratch = gradient_forms(units, parts)
    outs, sums = call(
        body,
        tiles,
        [full, kept, kept, wd, pl.BlockSpec(memory_space=pl.ANY)],
        outs,
        (dh, gate, up, w_down, at),
        riders,
        scratch=scratch,
        flops=6 * T * D * TILE * tiles,
        nbytes=8e6 * tiles,
        name="first_layer",
    )
    return [(outs[k : k + 3], outs[k + 3 : k + 6]) for k in range(0, 6 * units, 6)], sums


def gradient_out(riders, act, dy, parts):
    half = N // 2
    starts = [128 * sum(parts[:p]) for p in range(3)]
    rows = TILE // 2

    def body(act, dy, *outs):
        new = dot(act[...], dy[...], 0, 0).astype(BF16)
        for k in range(2):

            @pl.when((pl.program_id(0) >> 3) == k)
            def _():
                for q in range(2):
                    for p in range(3):
                        columns = slice(starts[p], starts[p] + 128 * parts[p])
                        outs[6 * q + 3 * k + p][...] = new[q * rows : (q + 1) * rows, columns]

    def out_spec(k, p):
        return pl.BlockSpec((None, rows, 128 * parts[p]), lambda i: (in_order(within(i, k * half, half), ORDERS[p]), 0, 0))

    outs, sums = call(
        body,
        N,
        [
            pl.BlockSpec((T, TILE), lambda i: (0, block_of(i & 7, lax.axis_index("dp"), 1 - (i >> 3)))),
            pl.BlockSpec((T, D), lambda i: (0, 0), pipeline_mode=pl.Buffered(1)),
        ],
        [(out_spec(k, p), shape((half, rows, 128 * parts[p]), BF16)) for q in range(2) for k in range(2) for p in range(3)],
        (act, dy),
        riders,
        flops=2 * T * D * FF,
        nbytes=33e6,
        name="gradient_out",
    )
    return [(outs[:3], outs[3:6]), (outs[6:9], outs[9:])], sums


def states_backward(riders, dgate, dup, w_gate, w_up, h, dy, number):
    wide = 512

    def body(dg, du, wg, wu, h, dy, out, by_gate, by_up, states, sem):
        i = pl.program_id(0)
        load = pltpu.make_async_copy(h, states, sem.at[0])
        put = pltpu.make_async_copy(states, out, sem.at[1])

        @pl.when(i == 0)
        def _():
            load.start()
            by_gate[...] = dot(dg[...], wg[...], 1, 1)
            by_up[...] = dot(du[...], wu[...], 1, 1)

        @pl.when(i > 0)
        def _():
            by_gate[...] += dot(dg[...], wg[...], 1, 1)
            by_up[...] += dot(du[...], wu[...], 1, 1)

        @pl.when(i == FF // wide - 1)
        def _():
            rows = 256
            load.wait()

            @pl.loop(0, T // rows)
            def _(r):
                at = pl.ds(pl.multiple_of(r * rows, rows), rows)
                da = (by_gate[at, :].astype(BF16) + by_up[at, :].astype(BF16)).astype(F32)
                x = states[at, :].astype(F32)
                scale = lax.rsqrt(jnp.mean(x**2, -1, keepdims=True) + 1e-6)
                along = jnp.mean(da * x, -1, keepdims=True)
                dx = da * scale - x * (scale**3 * along)
                states[at, :] = dy[at, :] + dx.astype(BF16)

            put.start()
            put.wait()

    full = pl.BlockSpec((T, D), lambda i: (0, 0), pipeline_mode=pl.Buffered(1))
    anywhere = pl.BlockSpec(memory_space=pl.ANY)
    tile = pl.BlockSpec((T, wide), lambda i: (0, i))
    w = pl.BlockSpec((None, D, wide), lambda i: (number, 0, i))
    (out,), sums = call(
        body,
        FF // wide,
        [tile, tile, w, w, anywhere, full],
        [(anywhere, shape((T, D), BF16))],
        (dgate, dup, w_gate, w_up, h, dy),
        riders,
        scratch=[pltpu.VMEM((T, D), F32)] * 2 + [pltpu.VMEM((T, D), BF16), pltpu.SemaphoreType.DMA((2,))],
        flops=4 * T * D * FF,
        nbytes=70e6,
        name="states_backward",
    )
    return out, sums


def update_in(place, sums, w_gate, w_up, m, v, number, first, tiles):
    steps, wide = 5, tiles * TILE
    rows, n = ROWS // steps, len(sums)

    def body(s, *refs):
        new, at = refs[-1], 0
        for q in range(n):
            for k in range(2):
                w, m, v = refs[n + 3 * (2 * q + k) :][:3]
                g = refs[q][:, k * wide : (k + 1) * wide]
                new[:, at : at + wide] = new_weight(w[...], m[...], v[...], g)
                at += wide

    def state(q):
        return pl.BlockSpec((None, rows, wide), lambda i, s: (number, i, first // tiles + q))

    def own(q):
        return pl.BlockSpec((None, rows, wide), lambda i, s: (number, s[0] * steps + i, first // tiles + q))

    return pl.pallas_call(
        body,
        grid_spec=pltpu.PrefetchScalarGridSpec(
            num_scalar_prefetch=1,
            grid=(steps,),
            in_specs=[pl.BlockSpec((rows, 2 * wide), lambda i, s: (i, 0))] * n
            + [spec for q in range(n) for _ in range(2) for spec in (own(q), state(q), state(q))],
            out_specs=pl.BlockSpec((rows, 2 * n * wide), lambda i, s: (i, 0)),
        ),
        out_shape=shape((ROWS, 2 * n * wide), BF16),
        compiler_params=params(),
        cost_estimate=cost(1e8, 1e7),
        name="update_in",
    )(place, *sums, *[t for q in range(n) for one in zip((w_gate, w_up), m, v) for t in one])


def update_out(place, sums, w_down, m, v, number):
    rows = TILE // 2

    def body(s, one, two, w, m, v, new):
        for q, g in enumerate((one, two)):

            @pl.when(pl.program_id(0) == q)
            def _():
                new[...] = new_weight(w[...], m[...], v[...], g[...])

    whole = pl.BlockSpec((rows, D), lambda i, s: (0, 0))
    state = pl.BlockSpec((None, rows, D), lambda i, s: (number, i, 0))
    own = pl.BlockSpec((None, rows, D), lambda i, s: (number, s[0] * 2 + i, 0))
    return pl.pallas_call(
        body,
        grid_spec=pltpu.PrefetchScalarGridSpec(
            num_scalar_prefetch=1,
            grid=(2,),
            in_specs=[whole, whole, own, state, state],
            out_specs=pl.BlockSpec((rows, D), lambda i, s: (i, 0)),
        ),
        out_shape=shape((TILE, D), BF16),
        compiler_params=params(),
        cost_estimate=cost(1e8, 1e7),
        name="update_out",
    )(place, *sums, w_down, m, v)


def lay_in(riders, gathered, outs, number, first, tiles):
    wide, rows = 512, 640
    each = tiles * TILE // wide
    blocks = gathered.shape[1] // 2 // wide

    def body(gate, up, *refs):
        refs[-2][...] = gate[...]
        refs[-1][...] = up[...]

    def place(i, upper):
        j = i // 2
        return (i % 2, (j // each) * 2 * each + upper * each + j % each)

    out = pl.BlockSpec((None, rows, wide), lambda i: (number, i % 2, first * TILE // wide + i // 2))
    return call(
        body,
        2 * blocks,
        [pl.BlockSpec((rows, wide), lambda i: place(i, 0)), pl.BlockSpec((rows, wide), lambda i: place(i, 1))]
        + [pl.BlockSpec(memory_space=pl.ANY)] * len(outs),
        [(out, shape((2, D, FF), BF16))] * 2,
        (gathered, gathered, *outs),
        riders,
        aliases={2: 0, 3: 1} if outs else {},
        flops=1e8,
        nbytes=2e7,
        name="lay_in",
    )


def lay_out(gathered, outs, number):
    rows = 512

    def body(new, *refs):
        refs[-1][...] = new[...]

    return pl.pallas_call(
        body,
        grid=(FF // rows,),
        in_specs=[pl.BlockSpec((rows, D), lambda i: (i, 0))] + [pl.BlockSpec(memory_space=pl.ANY)] * len(outs),
        out_specs=[pl.BlockSpec((None, rows, D), lambda i: (number, i, 0))],
        out_shape=[shape((2, FF, D), BF16)],
        input_output_aliases={1: 0} if outs else {},
        compiler_params=params(),
        cost_estimate=cost(1e8, 4 * D * FF),
        name="lay_out",
    )(gathered, *outs)


def moments(m, v, g):
    g = g.astype(F32)
    return 0.9 * m + 0.1 * g, 0.95 * v + 0.05 * g * g


def new_weight(w, m, v, g):
    m, v = moments(m, v, g)
    step = m * lax.rsqrt(v + 1e-8) + 0.1 * w.astype(F32)
    return (w.astype(F32) - 0.02 * step).astype(BF16)


class Line:
    def __init__(self):
        self.last = ()

    def run(self, f, first, *rest):
        first, self.last = lax.optimization_barrier((first, self.last))
        out = f(first, *rest)
        self.last = jax.tree.leaves(out)[-1:]
        return out


TILES = 4
PARTS = (3, 3, 2)
PARTS_OUT = ((4, 3, 3), (3, 4, 3))
UNITS = (2, 1, 1)
GROUPS = ((2, 1, 1), (2, 1, 1))


def solution(mesh):
    def step(x, dy, w_gate, w_up, w_down, *state):
        m, v = state[:3], state[3:]
        x, dy = x[0], dy[0]
        place = lax.axis_index("dp").astype(jnp.int32).reshape(1)
        line = Line()
        queue, done, lays = [], {}, []
        outs = {"in": [], "out": []}
        groups = [(number, "out", (0, 1)) for number in (0, 1)]
        for number in (0, 1):
            first = 0
            for size in GROUPS[number]:
                groups.append((number, "in", tuple(range(first, first + size))))
                first += size

        def only(riders, _):
            return call(None, 1, [], [], (), riders, name="exchange")

        def gather(number, kind, members):
            sums = [done[number, kind, one] for one in members]
            if kind == "in":
                first = members[0] * TILES
                new = line.run(update_in, place, sums, w_gate, w_up, m[:2], v[:2], number, first, TILES)
            else:
                new = line.run(update_out, place, sums, w_down, m[2], v[2], number)
            new = lax.all_gather(new, "dp", axis=0, tiled=True)

            def lay():
                if kind == "in":
                    outs["in"] = run(0, lay_in, new, outs["in"], number, first, TILES)
                else:
                    outs["out"] = line.run(lay_out, new, outs["out"], number)

            lays.append(lay)

        def run(room, f, *args):
            riding = queue[:room]
            del queue[:room]

            def beside(both, *rest):
                return f(both[0], *both[1], *rest)

            out, sums = line.run(beside, ([halves for _, halves in riding], args[:1]), *args[1:])
            for (name, _), one in zip(riding, sums):
                done[name] = one
            for group in list(groups):
                number, kind, members = group
                if all((number, kind, one) in done for one in members):
                    groups.remove(group)
                    gather(*group)
            return out

        a0, at0 = line.run(prepare, x)
        act0, gate0, up0 = line.run(forward, a0, w_gate, w_up, 0)
        h1, a1, at1 = line.run(down, act0, x, w_down, 0)
        at0, at1 = (t.reshape(N, ROWS, T) for t in (at0, at1))

        so_far = []
        for k in range(N // TILES):
            so_far, halves = run(1, last_layer, a1, at1, dy, w_gate, w_up, w_down, 1, k * TILES, TILES, PARTS, so_far)
            queue.append(((1, "in", k), halves))
        dgate, dup, act1 = so_far
        for k, halves in enumerate(run(1, gradient_out, act1, dy, PARTS_OUT[1])):
            queue.append(((1, "out", k), halves))
        dh1 = run(2, states_backward, dgate, dup, w_gate, w_up, h1, dy, 1)
        for k, halves in enumerate(run(1, gradient_out, act0, dh1, PARTS_OUT[0])):
            queue.append(((0, "out", k), halves))
        k = 0
        for units in UNITS:
            for halves in run(2, first_layer, dh1, at0, gate0, up0, w_down, 0, k * TILES, units, PARTS):
                queue.append(((0, "in", k), halves))
                k += 1
        while queue:
            run(2, only, place)
        while lays:
            lays.pop(0)()

        new_m, new_v = [], []
        for k in range(3):
            layers = []
            for number in range(2):
                if k == 2:
                    layers.append(jnp.concatenate([done[number, "out", q] for q in range(2)], axis=0))
                else:
                    columns = slice(k * TILES * TILE, (k + 1) * TILES * TILE)
                    layers.append(
                        jnp.concatenate([done[number, "in", q][:, columns] for q in range(N // TILES)], axis=1)
                    )
            one_m, one_v = moments(m[k], v[k], jnp.stack(layers))
            new_m.append(one_m)
            new_v.append(one_v)
        return (*outs["in"], *outs["out"], *new_m, *new_v)

    rows = P(None, "dp", None)
    return jax.shard_map(
        step,
        mesh=mesh,
        in_specs=(P(("rep", "dp")),) * 2 + (P(),) * 3 + (rows,) * 6,
        out_specs=(P("rep"),) * 3 + (P("rep", "dp", None),) * 6,
        check_vma=False,
    )
```
